1024 devices in a mesh: grp: 128 (over y, z), tp: 4 (over x_lo, core), fs: 2 (over x_hi).
Axes of the slice: x: 4 (x_hi: 2, x_lo: 2; x = x_hi * 2 + x_lo), y: 4, z: 32, core: 2. Of those that a mesh axis runs over, the one named last changes fastest.
Arguments:
- tokens: bfloat16 [8192, 4, 8192], P('grp', None, ('tp', 'fs')), may hold values from -64 to 64
- norm_gain: bfloat16 [8192], P(('tp', 'fs')), may hold values from 0.25 to 1.75
- queries: bfloat16 [8192, 4, 8192], P('grp', None, ('tp', 'fs')), may hold values from -64 to 64
- rotated_key_cache: bfloat16 [8192, 32, 1024], P('grp', None, ('tp', 'fs')), may hold values from -6 to 6
- head_value_cache: bfloat16 [8192, 32, 1024], P('grp', None, ('tp', 'fs')), may hold values from -6 to 6
- lengths: int32 [8192], P('grp'), may hold values from 2 to 32
- master: float32 [8192, 2048], P('grp', ('tp', 'fs')), may hold values from -0.0625 to 0.0625
- moment_first: float32 [8192, 2048], P('grp', ('tp', 'fs')), may hold values from -4 to 4
- moment_second: float32 [8192, 2048], P('grp', ('tp', 'fs')), may hold values from 0.1 to 1
- gradient: float32 [8192, 2048], P('grp', ('tp', 'fs')), may hold values from -6 to 6
Outputs:
- attended: bfloat16 [8192, 4, 8192], P('grp', None, ('tp', 'fs'))
- appended: bfloat16 [8192, 4, 2048], P('grp', None, ('tp', 'fs'))
- new_master: float32 [8192, 2048], P('grp', ('tp', 'fs'))
- new_first: float32 [8192, 2048], P('grp', ('tp', 'fs'))
- new_second: float32 [8192, 2048], P('grp', ('tp', 'fs'))
The draws below stay inside these ranges and needn't reach their ends.
All inputs are finite; a program needn't handle non-finite values.
Results may differ from the reference program's by a relative error of at most 0.0057.
Values may be sent and summed in bfloat16 or wider, within the bound.
No kernel may reach another device: no remote copies, remote signals or barrier semaphores. Data moves between devices by JAX's collectives and lax.ppermute only.
A program may use at most 64 MiB of HBM per device.

```python
import math
import jax
import jax.numpy as jnp
from jax import lax

MODEL_WIDTH = 8192
QUERY_HEADS = 64
KEY_VALUE_HEADS = 8
HEAD_SIZE = 128
REPLICA_ROWS = 64
CACHE_SLOTS = 32
NEW_TOKENS = 4
TOTAL_ROWS = 8192
KV_COLS = 2048
N_GRP = 128


def drawn_draw(key):
    cache_seed = jax.random.fold_in(key, 7001)
    query_seed = jax.random.fold_in(key, 7002)
    cache_dimensions = (TOTAL_ROWS, CACHE_SLOTS, KEY_VALUE_HEADS * HEAD_SIZE)
    query_shape = (TOTAL_ROWS, NEW_TOKENS, QUERY_HEADS * HEAD_SIZE)
    cache_key_seeds = jnp.clip(jax.random.normal(cache_seed, cache_dimensions, jnp.float32), -6.0, 6.0)
    query_draw = jnp.clip(jax.random.normal(query_seed, query_shape, jnp.float32), -6.0, 6.0)
    return (cache_key_seeds, query_draw)


def draw_rotated_key_cache(key, part):
    return drawn_draw(key)[0].astype(jnp.bfloat16)


def draw_queries(key, part):
    return drawn_draw(key)[1].astype(jnp.bfloat16)


def draw_tokens(key, part):
    base_seed = jax.random.fold_in(key, 8001)
    shape = (TOTAL_ROWS, NEW_TOKENS, MODEL_WIDTH)
    values = jnp.clip(jax.random.normal(base_seed, shape, jnp.float32), -6.0, 6.0)
    return values.astype(jnp.bfloat16)


def place_ends(result, stream_key, low, high):
    longest = result.shape.index(max(result.shape))
    spots = []
    for shift in (0, 1):
        where = [jax.random.randint(jax.random.fold_in(stream_key, axis), (), 0, length) for axis, length in enumerate(result.shape)]
        where[longest] = (where[longest] + shift) % result.shape[longest]
        spots.append(tuple(where))
    return result.at[spots[0]].set(low).at[spots[1]].set(high)


def block_levels(stream_key, shape, cuts, low, largest):
    def one(axis_at, blocks):
        steps = jax.random.uniform(jax.random.fold_in(jax.random.fold_in(stream_key, 6), axis_at), (blocks,), jnp.float32, low / len(cuts), largest / len(cuts))
        return jnp.repeat(jnp.exp(steps), shape[axis_at] // blocks).reshape((-1,) + (1,) * (len(shape) - axis_at - 1))

    factor_of = one(*cuts[0])
    for cut in cuts[1:]:
        factor_of = factor_of * one(*cut)
    return factor_of


def noise(key, shape, scale, limit, cuts=(), held_as=jnp.bfloat16):
    factor_of = block_levels(key, shape, cuts, -0.22, 0.18) if cuts else 1.0
    result = jax.random.normal(key, shape, jnp.float32) * scale * factor_of
    return jnp.minimum(jnp.maximum(result, -limit), limit).astype(held_as)


def setup_inputs(seed: int = 0) -> dict:
    splits = jax.random.split(jax.random.key(seed), 11)
    return {
        "tokens": draw_tokens(jax.random.fold_in(splits[10], 71), 0),
        "norm_gain": jnp.clip(1.0 + 0.15 * jax.random.normal(splits[1], (MODEL_WIDTH,), jnp.float32), 0.25, 1.75).astype(jnp.bfloat16),
        "queries": draw_queries(jax.random.fold_in(splits[10], 71), 0),
        "rotated_key_cache": draw_rotated_key_cache(jax.random.fold_in(splits[10], 71), 0),
        "head_value_cache": noise(splits[4], (TOTAL_ROWS, CACHE_SLOTS, KEY_VALUE_HEADS * HEAD_SIZE), 1.0, 6.0, ((0, 128), (2, 8))),
        "lengths": place_ends(jax.random.randint(splits[5], (TOTAL_ROWS,), 2, CACHE_SLOTS + 1), jax.random.fold_in(splits[5], 1), 2, CACHE_SLOTS).astype(jnp.int32),
        "master": noise(splits[6], (MODEL_WIDTH, KV_COLS), MODEL_WIDTH ** -0.5, 0.0625, ((0, 128), (1, 8)), jnp.float32),
        "moment_first": noise(splits[7], (MODEL_WIDTH, KV_COLS), 0.3, 4.0, ((0, 128), (1, 8)), jnp.float32),
        "moment_second": jnp.clip(jnp.exp(math.log(1.0) - 2.3025851 * jax.random.uniform(splits[8], (MODEL_WIDTH, KV_COLS), jnp.float32) ** block_levels(splits[8], (MODEL_WIDTH, KV_COLS), ((0, 128), (1, 8)), -0.2, 0.2)), 0.1, 1.0),
        "gradient": noise(splits[9], (MODEL_WIDTH, KV_COLS), 1.0, 6.0, ((0, 128), (1, 8)), jnp.float32),
    }


beta_first = 0.9
beta_second = 0.999
correct_first = 0.9999734386011124
correct_second = 0.09520785288629038
adam_eps = 1e-08
learn_rate = 0.003
decay_rate = 0.1
norm_eps = 1e-06
rope_base = 1000000.0

def rotate(keys, positions):
    halfway = keys.shape[-1] // 2
    frequency = rope_base ** (-(jnp.arange(halfway, dtype=jnp.float32) * 2.0 / keys.shape[-1]))
    angles = positions[:, :, None] * frequency[None, None, :]
    cosine = jnp.cos(angles)[:, :, None, :]
    sine = jnp.sin(angles)[:, :, None, :]
    first_half = keys[..., :halfway]
    second_half = keys[..., halfway:]
    return jnp.concatenate([first_half * cosine - second_half * sine, second_half * cosine + first_half * sine], axis=-1)

def attention(queries, rotated_key_cache, head_value_cache, key_new, value_new, lengths):
    batch_rows, steps = (queries.shape[0], queries.shape[1])
    window = rotated_key_cache.shape[1]
    kv_heads = rotated_key_cache.shape[2] // HEAD_SIZE
    sharing_factor = QUERY_HEADS // KEY_VALUE_HEADS
    factor = HEAD_SIZE ** (-0.5)
    query_heads = queries.reshape(batch_rows, steps, kv_heads, sharing_factor, HEAD_SIZE).astype(jnp.float32)
    cache_key_seeds = rotated_key_cache.reshape(batch_rows, window, kv_heads, HEAD_SIZE).astype(jnp.float32)
    cache_values = head_value_cache.reshape(batch_rows, window, kv_heads, HEAD_SIZE).astype(jnp.float32)
    scores_cached = jnp.einsum('rsxgd,rlxd->rxgsl', query_heads, cache_key_seeds) * factor
    scores_fresh = jnp.einsum('rsxgd,ruxd->rxgsu', query_heads, key_new.astype(jnp.float32)) * factor
    present = (jnp.arange(window, dtype=jnp.int32)[None, :] < lengths[:, None])[:, None, None, None, :]
    causal = (jnp.arange(steps, dtype=jnp.int32)[None, :] <= jnp.arange(steps, dtype=jnp.int32)[:, None])[None, None, None, :, :]
    scores_cached = jnp.where(present, scores_cached, -jnp.inf)
    scores_fresh = jnp.where(causal, scores_fresh, -jnp.inf)
    ceiling = jnp.maximum(lax.optimization_barrier(jnp.max(scores_cached, axis=-1, keepdims=True)), lax.optimization_barrier(jnp.max(scores_fresh, axis=-1, keepdims=True)))
    probs_cached = jnp.exp(scores_cached - ceiling)
    probs_fresh = jnp.exp(scores_fresh - ceiling)
    denom = lax.optimization_barrier(jnp.sum(probs_cached, axis=-1, keepdims=True)) + lax.optimization_barrier(jnp.sum(probs_fresh, axis=-1, keepdims=True))
    weights_cached = probs_cached.astype(jnp.bfloat16).astype(jnp.float32)
    weights_fresh = probs_fresh.astype(jnp.bfloat16).astype(jnp.float32)
    blended = jnp.einsum('rxgsl,rlxd->rsxgd', weights_cached, cache_values)
    blended = blended + jnp.einsum('rxgsu,ruxd->rsxgd', weights_fresh, value_new.astype(jnp.float32))
    blended = blended / jnp.transpose(denom, (0, 3, 1, 2, 4))
    return blended.astype(jnp.bfloat16).reshape(batch_rows, steps, kv_heads * sharing_factor * HEAD_SIZE)

def reference(tokens, norm_gain, queries, rotated_key_cache, head_value_cache, lengths, master, moment_first, moment_second, gradient):
    average = beta_first * moment_first + (1.0 - beta_first) * gradient
    variance = beta_second * moment_second + (1.0 - beta_second) * gradient * gradient
    update = average / correct_first / (jnp.sqrt(variance / correct_second) + adam_eps)
    renewed = master - learn_rate * (update + decay_rate * master)
    layer_half = renewed.astype(jnp.bfloat16)
    gain_wide = norm_gain.astype(jnp.float32)

    def replica(bundle):
        replica_tokens, replica_queries, replica_keys, replica_values, replica_lengths = bundle
        widened = replica_tokens.astype(jnp.float32)
        mean_square = lax.optimization_barrier(jnp.sum(widened * widened, axis=-1, keepdims=True)) / MODEL_WIDTH
        normed = (widened * lax.rsqrt(mean_square + norm_eps) * gain_wide).astype(jnp.bfloat16)
        projected_output = jnp.dot(normed.reshape(REPLICA_ROWS * NEW_TOKENS, MODEL_WIDTH), layer_half, preferred_element_type=jnp.float32)
        projected_output = projected_output.reshape(REPLICA_ROWS, NEW_TOKENS, KEY_VALUE_HEADS, 2, HEAD_SIZE)
        positions = (replica_lengths[:, None] + jnp.arange(NEW_TOKENS, dtype=jnp.int32)[None, :]).astype(jnp.float32)
        key_new = rotate(projected_output[:, :, :, 0, :], positions).astype(jnp.bfloat16)
        value_new = projected_output[:, :, :, 1, :].astype(jnp.bfloat16)
        appended = jnp.stack([key_new, value_new], axis=3).reshape(REPLICA_ROWS, NEW_TOKENS, KV_COLS)
        attended = attention(replica_queries, replica_keys, replica_values, key_new, value_new, replica_lengths)
        return (attended, appended)
    grouped_bundles = (tokens.reshape(N_GRP, REPLICA_ROWS, NEW_TOKENS, MODEL_WIDTH), queries.reshape(N_GRP, REPLICA_ROWS, NEW_TOKENS, QUERY_HEADS * HEAD_SIZE), rotated_key_cache.reshape(N_GRP, REPLICA_ROWS, CACHE_SLOTS, KEY_VALUE_HEADS * HEAD_SIZE), head_value_cache.reshape(N_GRP, REPLICA_ROWS, CACHE_SLOTS, KEY_VALUE_HEADS * HEAD_SIZE), lengths.reshape(N_GRP, REPLICA_ROWS))
    attended, appended = lax.map(replica, grouped_bundles)
    attended = attended.reshape(TOTAL_ROWS, NEW_TOKENS, QUERY_HEADS * HEAD_SIZE)
    appended = appended.reshape(TOTAL_ROWS, NEW_TOKENS, KV_COLS)
    return (attended, appended, renewed, average, variance)
```

```python
import functools

import jax
import jax.numpy as jnp
from jax import lax
from jax.experimental import pallas as pl
from jax.experimental.pallas import tpu as pltpu
from jax.sharding import Mesh
from jax.sharding import PartitionSpec as P

MODEL_WIDTH = 8192
QUERY_HEADS = 64
KEY_VALUE_HEADS = 8
HEAD_SIZE = 128
GRP = ("y", "zh", "zl")
Z = ("zh", "zl")
COLS = ("xl", "c", "xh")


beta_first = 0.9
beta_second = 0.999
correct_first = 0.9999734386011124
correct_second = 0.09520785288629038
adam_eps = 1e-08
learn_rate = 0.003
decay_rate = 0.1
norm_eps = 1e-06
rope_base = 1000000.0

TOKENS = 256
EXTRA = 16
SLICE = 1024
SHIFTS = (0, 1, 2, 3)


def sums_block(sums):
    high = sums.astype(jnp.bfloat16).astype(jnp.float32)
    low = sums - high
    row = lax.broadcasted_iota(jnp.int32, (EXTRA, sums.shape[1]), 0)
    return jnp.where(row == 0, high, jnp.where(row == 1, low, 0.0)).astype(jnp.bfloat16)


def prepare_kernel(tokens_ref, gain_ref, out_ref):
    wide = tokens_ref[...].astype(jnp.float32)
    out_ref[:TOKENS, :] = (wide * gain_ref[...].astype(jnp.float32)).astype(jnp.bfloat16)
    sums = jnp.sum(wide * wide, axis=1, keepdims=True)
    sums = jnp.transpose(jnp.broadcast_to(sums, (TOKENS, 128)))[:1, :]
    out_ref[TOKENS:, :TOKENS] = sums_block(sums)
    out_ref[TOKENS:, TOKENS:] = jnp.zeros((EXTRA, SLICE - TOKENS), jnp.bfloat16)


def prepare(tokens, gain):
    return pl.pallas_call(
        prepare_kernel,
        out_shape=jax.ShapeDtypeStruct((TOKENS + EXTRA, SLICE), jnp.bfloat16),
        name="prepare",
    )(tokens, gain)


def project_kernel(own_ref, other_ref, *refs):
    w_refs, out_ref, layer = refs[:4], refs[4], refs[5]
    zl, core = lax.axis_index("zl"), lax.axis_index("c")
    x = lax.axis_index("xh") * 2 + lax.axis_index("xl")
    for d, w_ref in zip(SHIFTS, w_refs):
        place = lax.rem(zl + 4 - d, 4)
        layer[:, :, place] = w_ref[...].reshape(2, 4, 64, 256)
    for a_ref, c in ((own_ref, core), (other_ref, 1 - core)):
        for low in range(2):
            slots = [lax.rem(x + 4 - (2 * high + low), 4) for high in range(2)]
            total = jnp.zeros((TOKENS, 256), jnp.float32)
            sums = jnp.zeros((1, TOKENS), jnp.float32)
            for high, slot in enumerate(slots):
                total += jnp.dot(
                    a_ref[slot, :TOKENS, :],
                    layer[high].reshape(SLICE, 256),
                    preferred_element_type=jnp.float32,
                )
                tail = a_ref[slot, TOKENS:, :TOKENS].astype(jnp.float32)
                sums += tail[0:1] + tail[1:2]
            out_ref[2 * low + c, :TOKENS, :] = total.astype(jnp.bfloat16)
            out_ref[2 * low + c, TOKENS:, :] = sums_block(sums)


def project(own, other, blocks):
    return pl.pallas_call(
        project_kernel,
        out_shape=jax.ShapeDtypeStruct((4, TOKENS + EXTRA, 256), jnp.bfloat16),
        scratch_shapes=[pltpu.VMEM((2, 4, 4, 64, 256), jnp.bfloat16)],
        name="project",
    )(own, other, *blocks)


def rotate(keys, positions):
    halfway = keys.shape[-1] // 2
    frequency = rope_base ** (-(jnp.arange(halfway, dtype=jnp.float32) * 2.0 / keys.shape[-1]))
    angles = positions[:, :, None] * frequency[None, None, :]
    cosine = jnp.cos(angles)[:, :, None, :]
    sine = jnp.sin(angles)[:, :, None, :]
    first_half = keys[..., :halfway]
    second_half = keys[..., halfway:]
    return jnp.concatenate(
        [first_half * cosine - second_half * sine, second_half * cosine + first_half * sine],
        axis=-1,
    )


def attention(queries, rotated_key_cache, head_value_cache, key_new, value_new, lengths):
    batch_rows, steps = (queries.shape[0], queries.shape[1])
    window = rotated_key_cache.shape[1]
    kv_heads = rotated_key_cache.shape[2] // HEAD_SIZE
    sharing_factor = QUERY_HEADS // KEY_VALUE_HEADS
    factor = HEAD_SIZE ** (-0.5)
    query_heads = queries.reshape(batch_rows, steps, kv_heads, sharing_factor, HEAD_SIZE)
    cache_key_seeds = rotated_key_cache.reshape(batch_rows, window, kv_heads, HEAD_SIZE)
    cache_values = head_value_cache.reshape(batch_rows, window, kv_heads, HEAD_SIZE)
    scores_cached = (
        jnp.einsum(
            "rsxgd,rlxd->rxgsl", query_heads, cache_key_seeds, preferred_element_type=jnp.float32
        )
        * factor
    )
    scores_fresh = (
        jnp.einsum("rsxgd,ruxd->rxgsu", query_heads, key_new, preferred_element_type=jnp.float32)
        * factor
    )
    present = (jnp.arange(window, dtype=jnp.int32)[None, :] < lengths[:, None])[
        :, None, None, None, :
    ]
    causal = (
        jnp.arange(steps, dtype=jnp.int32)[None, :] <= jnp.arange(steps, dtype=jnp.int32)[:, None]
    )[None, None, None, :, :]
    scores_cached = jnp.where(present, scores_cached, -jnp.inf)
    scores_fresh = jnp.where(causal, scores_fresh, -jnp.inf)
    ceiling = jnp.maximum(
        jnp.max(scores_cached, axis=-1, keepdims=True),
        jnp.max(scores_fresh, axis=-1, keepdims=True),
    )
    probs_cached = jnp.exp(scores_cached - ceiling)
    probs_fresh = jnp.exp(scores_fresh - ceiling)
    denom = jnp.sum(probs_cached, axis=-1, keepdims=True) + jnp.sum(
        probs_fresh, axis=-1, keepdims=True
    )
    weights_cached = probs_cached.astype(jnp.bfloat16)
    weights_fresh = probs_fresh.astype(jnp.bfloat16)
    blended = jnp.einsum(
        "rxgsl,rlxd->rsxgd", weights_cached, cache_values, preferred_element_type=jnp.float32
    )
    blended = blended + jnp.einsum(
        "rxgsu,ruxd->rsxgd", weights_fresh, value_new, preferred_element_type=jnp.float32
    )
    blended = blended / jnp.transpose(denom, (0, 3, 1, 2, 4))
    return blended.astype(jnp.bfloat16).reshape(
        batch_rows, steps, kv_heads * sharing_factor * HEAD_SIZE
    )


def along_x(array, shift):
    at = [(x % 2) * 2 + x // 2 for x in range(4)]
    return lax.ppermute(array, ("xl", "xh"), [(at[x], at[(x + shift) % 4]) for x in range(4)])


def along_z(array, shift):
    return lax.ppermute(array, Z, [(z, (z + shift) % 32) for z in range(32)])


def shards(
    tokens,
    norm_gain,
    queries,
    rotated_key_cache,
    head_value_cache,
    lengths,
    master,
    moment_first,
    moment_second,
    gradient,
):
    batch_rows, steps = (tokens.shape[0], tokens.shape[1])
    packed = prepare(tokens.reshape(TOKENS, SLICE), norm_gain.reshape(1, SLICE))
    turned = lax.ppermute(
        packed, ("y", "xl", "c"), [(a * 4 + b, b * 4 + a) for a in range(4) for b in range(4)]
    )
    average = beta_first * moment_first + (1.0 - beta_first) * gradient
    variance = beta_second * moment_second + (1.0 - beta_second) * gradient * gradient
    update = average / correct_first / (jnp.sqrt(variance / correct_second) + adam_eps)
    renewed = master - learn_rate * (update + decay_rate * master)
    layer_half = renewed.astype(jnp.bfloat16)
    columns = layer_half.shape[1]
    spread = lax.all_to_all(jnp.broadcast_to(layer_half[None], (8, 64, columns)), "zh", 0, 0)
    spread = spread.reshape(512, columns)
    own = jnp.stack([turned] + [along_x(turned, d) for d in SHIFTS[1:]])
    other = lax.ppermute(own, "c", [(0, 1), (1, 0)])
    blocks = [spread] + [along_z(spread, d) for d in (1, 2, 31)]
    partial = project(own, other, blocks)
    parts = lax.all_to_all(partial, "y", 0, 0)
    sums = jnp.sum(parts[:, TOKENS : TOKENS + 2, :].astype(jnp.float32), axis=(0, 1))
    scale = lax.rsqrt(sums / MODEL_WIDTH + norm_eps)
    projected_output = jnp.sum(parts[:, :TOKENS, :].astype(jnp.float32), axis=0) * scale[:, None]
    kv_heads = columns // (2 * HEAD_SIZE)
    projected_output = projected_output.reshape(batch_rows, steps, kv_heads, 2, HEAD_SIZE)
    positions = (lengths[:, None] + jnp.arange(steps, dtype=jnp.int32)[None, :]).astype(jnp.float32)
    key_new = rotate(projected_output[:, :, :, 0, :], positions).astype(jnp.bfloat16)
    value_new = projected_output[:, :, :, 1, :].astype(jnp.bfloat16)
    appended = jnp.stack([key_new, value_new], axis=3).reshape(batch_rows, steps, columns)
    attended = attention(queries, rotated_key_cache, head_value_cache, key_new, value_new, lengths)
    return (attended, appended, renewed, average, variance)


def solution(mesh):
    split = Mesh(
        mesh.devices.reshape(4, 8, 4, 2, 2, 2),
        ("y", "zh", "zl", "xl", "c", "xh"),
    )
    placed = (
        P(GRP, None, COLS),
        P(COLS),
        P(GRP, None, COLS),
        P(GRP, None, COLS),
        P(GRP, None, COLS),
        P(GRP),
        P(GRP, COLS),
        P(GRP, COLS),
        P(GRP, COLS),
        P(GRP, COLS),
    )
    return jax.shard_map(
        shards,
        mesh=split,
        in_specs=placed,
        out_specs=(
            P(GRP, None, COLS),
            P(GRP, None, COLS),
            P(GRP, COLS),
            P(GRP, COLS),
            P(GRP, COLS),
        ),
        check_vma=False,
    )
```

```python
import jax
import jax.numpy as jnp
from jax import lax
from jax.experimental import pallas as pl
from jax.experimental.pallas import tpu as pltpu
from jax.sharding import Mesh
from jax.sharding import PartitionSpec as P


MODEL_WIDTH = 8192
HEAD_SIZE = 128
GRP = ("y", "far", "near")
Z = ("far", "near")
COLS = ("xl", "c", "xh")


beta_first = 0.9
beta_second = 0.999
correct_first = 0.9999734386011124
correct_second = 0.09520785288629038
adam_eps = 1e-08
learn_rate = 0.003
decay_rate = 0.1
norm_eps = 1e-06
rope_base = 1000000.0

TOKENS = 256
EXTRA = 16
SLICE = 1024
CACHE_SLOTS = 32


def sums_block(sums):
    high = sums.astype(jnp.bfloat16).astype(jnp.float32)
    low = sums - high
    row = lax.broadcasted_iota(jnp.int32, (EXTRA, sums.shape[1]), 0)
    return jnp.where(row == 0, high, jnp.where(row == 1, low, 0.0)).astype(jnp.bfloat16)


def prepare_kernel(tokens_ref, gain_ref, out_ref):
    wide = tokens_ref[...].astype(jnp.float32)
    out_ref[:TOKENS, :] = (wide * gain_ref[...].astype(jnp.float32)).astype(jnp.bfloat16)
    sums = jnp.sum(wide * wide, axis=1, keepdims=True)
    sums = jnp.transpose(jnp.broadcast_to(sums, (TOKENS, 128)))[:1, :]
    out_ref[TOKENS:, :TOKENS] = sums_block(sums)
    out_ref[TOKENS:, TOKENS:] = jnp.zeros((EXTRA, SLICE - TOKENS), jnp.bfloat16)


def prepare(tokens, gain):
    return pl.pallas_call(
        prepare_kernel,
        out_shape=jax.ShapeDtypeStruct((TOKENS + EXTRA, SLICE), jnp.bfloat16),
        compiler_params=pltpu.CompilerParams(vmem_limit_bytes=8 << 20),
        name="prepare",
    )(tokens, gain)


def join_kernel(*refs):
    *parts, out_ref = refs
    for k, part in enumerate(parts):
        out_ref[256 * k : 256 * (k + 1), :] = part[...]


def joined(*parts):
    return pl.pallas_call(
        join_kernel,
        out_shape=jax.ShapeDtypeStruct((256 * len(parts), 256), jnp.bfloat16),
        compiler_params=pltpu.CompilerParams(vmem_limit_bytes=2 << 20),
        name="joined",
    )(*parts)


def project_kernel(own_ref, other_ref, *refs):
    w_refs, out_ref, layer = refs[:3], refs[3], refs[4]
    near, core = lax.axis_index("near"), lax.axis_index("c")
    x = lax.axis_index("xh") * 2 + lax.axis_index("xl")
    for w_ref, offsets in zip(w_refs, ((0, 5, 3), (7, 4, 2), (1, 6, 4))):
        for k, offset in enumerate(offsets):
            place = lax.rem(near + offset, 8)
            layer[:, :, place] = w_ref[256 * k : 256 * (k + 1), :].reshape(2, 2, 64, 256)
    for a_ref, c in ((own_ref, core), (other_ref, 1 - core)):
        for low in range(2):
            slots = [lax.rem(x + 4 - (2 * high + low), 4) for high in range(2)]
            total = jnp.zeros((TOKENS, 256), jnp.float32)
            sums = jnp.zeros((1, TOKENS), jnp.float32)
            for high, slot in enumerate(slots):
                total += jnp.dot(
                    a_ref[slot, :TOKENS, :],
                    layer[high].reshape(SLICE, 256),
                    preferred_element_type=jnp.float32,
                )
                tail = a_ref[slot, TOKENS:, :TOKENS].astype(jnp.float32)
                sums += tail[0:1] + tail[1:2]
            out_ref[2 * low + c, :TOKENS, :] = total.astype(jnp.bfloat16)
            out_ref[2 * low + c, TOKENS:, :] = sums_block(sums)


def project(own, other, blocks):
    return pl.pallas_call(
        project_kernel,
        out_shape=jax.ShapeDtypeStruct((4, TOKENS + EXTRA, 256), jnp.bfloat16),
        scratch_shapes=[pltpu.VMEM((2, 2, 8, 64, 256), jnp.bfloat16)],
        compiler_params=pltpu.CompilerParams(vmem_limit_bytes=16 << 20),
        name="project",
    )(own, other, *blocks)


def group_queries(queries_ref, group):
    at = pl.ds(16 * group, 16)
    return jnp.concatenate(
        [queries_ref[at, pl.ds(HEAD_SIZE * head, HEAD_SIZE)] for head in range(8)], axis=0
    )


def cached_kernel(lengths_ref, queries_ref, keys_ref, values_ref, sums_ref, stats_ref):
    row = lax.broadcasted_iota(jnp.int32, (128, 128), 0)
    lane = lax.broadcasted_iota(jnp.int32, (128, 128), 1)
    same_row = (row // 4) % 4 == lane // CACHE_SLOTS
    for group in range(16):
        at = pl.ds(128 * group, 128)
        longest = jnp.zeros((128, 128), jnp.int32)
        for k in range(4):
            longest = jnp.where(lane // CACHE_SLOTS == k, lengths_ref[4 * group + k], longest)
        scores = lax.dot_general(
            group_queries(queries_ref, group),
            keys_ref[at, :],
            (((1,), (1,)), ((), ())),
            preferred_element_type=jnp.float32,
        ) * (HEAD_SIZE**-0.5)
        scores = jnp.where(same_row & (lane % CACHE_SLOTS < longest), scores, -jnp.inf)
        top = jnp.max(scores, axis=1, keepdims=True)
        probs = jnp.exp(scores - top)
        total = jnp.sum(probs, axis=1, keepdims=True)
        sums_ref[at, :] = jnp.dot(
            probs.astype(jnp.bfloat16), values_ref[at, :], preferred_element_type=jnp.float32
        )
        stats_ref[:, group : group + 1] = top
        stats_ref[:, 16 + group : 17 + group] = total


def cached_part(lengths, queries, keys, values):
    vmem = pl.BlockSpec(memory_space=pltpu.VMEM)
    return pl.pallas_call(
        cached_kernel,
        in_specs=[pl.BlockSpec(memory_space=pltpu.SMEM), vmem, vmem, vmem],
        out_shape=[
            jax.ShapeDtypeStruct((2048, HEAD_SIZE), jnp.float32),
            jax.ShapeDtypeStruct((128, 128), jnp.float32),
        ],
        compiler_params=pltpu.CompilerParams(vmem_limit_bytes=12 << 20),
        cost_estimate=pl.CostEstimate(flops=150_000_000, bytes_accessed=3 << 20, transcendentals=1 << 18),
        name="cached",
    )(lengths, queries, keys, values)


def finish_kernel(
    parts_ref, cosine_ref, sine_ref, queries_ref, sums_ref, stats_ref, attended_ref, appended_ref
):
    total = jnp.zeros((TOKENS, 256), jnp.float32)
    sums = jnp.zeros((1, TOKENS), jnp.float32)
    for k in range(4):
        total += parts_ref[k, :TOKENS, :].astype(jnp.float32)
        tail = parts_ref[k, TOKENS:, :].astype(jnp.float32)
        sums += tail[0:1] + tail[1:2]
    scale = lax.rsqrt(sums / MODEL_WIDTH + norm_eps)
    scale = jnp.transpose(jnp.broadcast_to(scale, (HEAD_SIZE, TOKENS)))
    keys = total[:, :HEAD_SIZE] * scale
    keys = keys * cosine_ref[...] + pltpu.roll(keys, HEAD_SIZE // 2, 1) * sine_ref[...]
    keys = keys.astype(jnp.bfloat16)
    values = (total[:, HEAD_SIZE:] * scale).astype(jnp.bfloat16)
    appended_ref[:, :, :HEAD_SIZE] = keys.reshape(64, 4, HEAD_SIZE)
    appended_ref[:, :, HEAD_SIZE:] = values.reshape(64, 4, HEAD_SIZE)
    row = lax.broadcasted_iota(jnp.int32, (128, 16), 0)
    lane = lax.broadcasted_iota(jnp.int32, (128, 16), 1)
    seen = ((row // 4) % 4 == lane // 4) & (lane % 4 <= row % 4)
    for group in range(16):
        at = pl.ds(128 * group, 128)
        near = slice(16 * group, 16 * group + 16)
        scores = lax.dot_general(
            group_queries(queries_ref, group),
            keys[near],
            (((1,), (1,)), ((), ())),
            preferred_element_type=jnp.float32,
        ) * (HEAD_SIZE**-0.5)
        scores = jnp.where(seen, scores, -jnp.inf)
        old_top = stats_ref[:, group : group + 1]
        old_total = stats_ref[:, 16 + group : 17 + group]
        top = jnp.maximum(jnp.max(scores, axis=1, keepdims=True), old_top)
        probs = jnp.exp(scores - top)
        factor = jnp.exp(old_top - top)
        denom = jnp.sum(probs, axis=1, keepdims=True) + old_total * factor
        blended = sums_ref[at, :] * factor + jnp.dot(
            probs.astype(jnp.bfloat16), values[near], preferred_element_type=jnp.float32
        )
        blended = (blended / denom).astype(jnp.bfloat16)
        for head in range(8):
            attended_ref[4 * group : 4 * group + 4, :, HEAD_SIZE * head : HEAD_SIZE * (head + 1)] = (
                blended[16 * head : 16 * head + 16].reshape(4, 4, HEAD_SIZE)
            )


def finish(parts, cosine, sine, queries, sums, stats):
    return pl.pallas_call(
        finish_kernel,
        out_shape=[
            jax.ShapeDtypeStruct((TOKENS // 4, 4, SLICE), jnp.bfloat16),
            jax.ShapeDtypeStruct((TOKENS // 4, 4, 256), jnp.bfloat16),
        ],
        compiler_params=pltpu.CompilerParams(vmem_limit_bytes=12 << 20),
        name="finish",
    )(parts, cosine, sine, queries, sums, stats)


def turns(lengths, steps):
    half = HEAD_SIZE // 2
    frequency = rope_base ** (-(jnp.arange(half, dtype=jnp.float32) * 2.0 / HEAD_SIZE))
    positions = (lengths[:, None] + jnp.arange(steps, dtype=jnp.int32)[None, :]).astype(jnp.float32)
    angles = positions.reshape(-1)[:, None] * frequency[None, :]
    cosine, sine = jnp.cos(angles), jnp.sin(angles)
    return jnp.concatenate([cosine, cosine], axis=1), jnp.concatenate([-sine, sine], axis=1)


def along_x(array, shift):
    at = [(x % 2) * 2 + x // 2 for x in range(4)]
    return lax.ppermute(array, ("xl", "xh"), [(at[x], at[(x + shift) % 4]) for x in range(4)])


def along_z(array, shift):
    return lax.ppermute(array, Z, [(z, (z + shift) % 32) for z in range(32)])


def shards(
    tokens,
    norm_gain,
    queries,
    rotated_key_cache,
    head_value_cache,
    lengths,
    master,
    moment_first,
    moment_second,
    gradient,
):
    batch_rows, steps = (tokens.shape[0], tokens.shape[1])
    exchange = [(a * 4 + b, b * 4 + a) for a in range(4) for b in range(4)]
    turned = lax.ppermute(tokens, ("y", "xl", "c"), exchange)
    gain = lax.ppermute(norm_gain.reshape(1, SLICE), ("y", "xl", "c"), exchange)
    turned = prepare(turned.reshape(TOKENS, SLICE), gain)
    average = beta_first * moment_first + (1.0 - beta_first) * gradient
    variance = beta_second * moment_second + (1.0 - beta_second) * gradient * gradient
    update = average / correct_first / (jnp.sqrt(variance / correct_second) + adam_eps)
    renewed = master - learn_rate * (update + decay_rate * master)
    layer_half = renewed.astype(jnp.bfloat16)
    columns = layer_half.shape[1]
    spread = lax.all_to_all(jnp.broadcast_to(layer_half[None], (4, 64, columns)), "far", 0, 0)
    spread = spread.reshape(256, columns)
    ring = []
    for d in (2, 1, 3):
        ring.append(along_x(turned, d))
    own = jnp.stack([turned, ring[1], ring[0], ring[2]])
    other = lax.ppermute(own, "c", [(0, 1), (1, 0)])
    below = along_z(spread, 3)
    above = along_z(spread, 29)
    held = joined(spread, below, above)
    from_below = along_z(held, 1)
    from_above = along_z(held, 31)
    queries_flat = queries.reshape(TOKENS, SLICE)
    old_sums, old_stats = cached_part(
        lengths,
        queries_flat,
        rotated_key_cache.reshape(batch_rows * CACHE_SLOTS, HEAD_SIZE),
        head_value_cache.reshape(batch_rows * CACHE_SLOTS, HEAD_SIZE),
    )
    cosine, sine = turns(lengths, steps)
    partial = project(own, other, [held, from_below, from_above])
    parts = lax.all_to_all(partial, "y", 0, 0)
    attended, appended = finish(parts, cosine, sine, queries_flat, old_sums, old_stats)
    return (
        attended,
        appended,
        renewed,
        average,
        variance,
    )


def solution(mesh):
    split = Mesh(
        mesh.devices.reshape(4, 4, 8, 2, 2, 2),
        ("y", "far", "near", "xl", "c", "xh"),
    )
    placed = (
        P(GRP, None, COLS),
        P(COLS),
        P(GRP, None, COLS),
        P(GRP, None, COLS),
        P(GRP, None, COLS),
        P(GRP),
        P(GRP, COLS),
        P(GRP, COLS),
        P(GRP, COLS),
        P(GRP, COLS),
    )
    return jax.shard_map(
        shards,
        mesh=split,
        in_specs=placed,
        out_specs=(
            P(GRP, None, COLS),
            P(GRP, None, COLS),
            P(GRP, COLS),
            P(GRP, COLS),
            P(GRP, COLS),
        ),
        check_vma=False,
    )
```

```python
import jax
import jax.numpy as jnp
from jax import lax
from jax.experimental import pallas as pl
from jax.experimental.pallas import tpu as pltpu
from jax.sharding import Mesh
from jax.sharding import PartitionSpec as P


MODEL_WIDTH = 8192
HEAD_SIZE = 128
GRP = ("y", "far", "near")
Z = ("far", "near")
COLS = ("xl", "c", "xh")


beta_first = 0.9
beta_second = 0.999
correct_first = 0.9999734386011124
correct_second = 0.09520785288629038
adam_eps = 1e-08
learn_rate = 0.003
decay_rate = 0.1
norm_eps = 1e-06
rope_base = 1000000.0

TOKENS = 256
EXTRA = 16
SLICE = 1024
CACHE_SLOTS = 32


def sums_block(sums):
    high = sums.astype(jnp.bfloat16).astype(jnp.float32)
    low = sums - high
    row = lax.broadcasted_iota(jnp.int32, (EXTRA, sums.shape[1]), 0)
    return jnp.where(row == 0, high, jnp.where(row == 1, low, 0.0)).astype(jnp.bfloat16)


def prepare_kernel(tokens_ref, gain_ref, out_ref):
    wide = tokens_ref[...].astype(jnp.float32)
    out_ref[:TOKENS, :] = (wide * gain_ref[...].astype(jnp.float32)).astype(jnp.bfloat16)
    sums = jnp.sum(wide * wide, axis=1, keepdims=True)
    sums = jnp.transpose(jnp.broadcast_to(sums, (TOKENS, 128)))[:1, :]
    out_ref[TOKENS:, :TOKENS] = sums_block(sums)
    out_ref[TOKENS:, TOKENS:] = jnp.zeros((EXTRA, SLICE - TOKENS), jnp.bfloat16)


def prepare(tokens, gain):
    return pl.pallas_call(
        prepare_kernel,
        out_shape=jax.ShapeDtypeStruct((TOKENS + EXTRA, SLICE), jnp.bfloat16),
        compiler_params=pltpu.CompilerParams(vmem_limit_bytes=8 << 20),
        name="prepare",
    )(tokens, gain)


def join_kernel(own_ref, below_ref, above_ref, up_ref, down_ref):
    for out_ref, first, second, rows in (
        (up_ref, above_ref, below_ref, slice(0, 128)),
        (down_ref, below_ref, above_ref, slice(128, 256)),
    ):
        out_ref[:256, :] = own_ref[...]
        out_ref[256:512, :] = first[...]
        out_ref[512:, :] = second[rows, :]


def joined(own, below, above):
    return pl.pallas_call(
        join_kernel,
        out_shape=[jax.ShapeDtypeStruct((640, 256), jnp.bfloat16)] * 2,
        compiler_params=pltpu.CompilerParams(vmem_limit_bytes=4 << 20),
        name="joined",
    )(own, below, above)


def project_kernel(own_ref, other_ref, *refs):
    up_ref, down_ref, below_ref, above_ref, out_ref, layer = refs
    near, core = lax.axis_index("near"), lax.axis_index("c")
    x = lax.axis_index("xh") * 2 + lax.axis_index("xl")
    for ref, at, offset in (
        (down_ref, 0, 0),
        (down_ref, 256, 5),
        (up_ref, 256, 3),
        (below_ref, 0, 7),
        (below_ref, 256, 2),
        (above_ref, 0, 1),
        (above_ref, 256, 6),
    ):
        layer[:, :, lax.rem(near + offset, 8)] = ref[at : at + 256, :].reshape(2, 2, 64, 256)
    for half, ref in enumerate((below_ref, above_ref)):
        layer[half, :, lax.rem(near + 4, 8)] = ref[512:, :].reshape(2, 64, 256)
    for a_ref, c in ((own_ref, core), (other_ref, 1 - core)):
        for low in range(2):
            slots = [lax.rem(x + 4 - (2 * high + low), 4) for high in range(2)]
            total = jnp.zeros((TOKENS, 256), jnp.float32)
            sums = jnp.zeros((1, TOKENS), jnp.float32)
            for high, slot in enumerate(slots):
                total += jnp.dot(
                    a_ref[slot, :TOKENS, :],
                    layer[high].reshape(SLICE, 256),
                    preferred_element_type=jnp.float32,
                )
                tail = a_ref[slot, TOKENS:, :TOKENS].astype(jnp.float32)
                sums += tail[0:1] + tail[1:2]
            out_ref[2 * low + c, :TOKENS, :] = total.astype(jnp.bfloat16)
            out_ref[2 * low + c, TOKENS:, :] = sums_block(sums)


def project(own, other, blocks):
    return pl.pallas_call(
        project_kernel,
        out_shape=jax.ShapeDtypeStruct((4, TOKENS + EXTRA, 256), jnp.bfloat16),
        scratch_shapes=[pltpu.VMEM((2, 2, 8, 64, 256), jnp.bfloat16)],
        compiler_params=pltpu.CompilerParams(vmem_limit_bytes=16 << 20),
        name="project",
    )(own, other, *blocks)


def group_queries(queries_ref, group):
    at = pl.ds(16 * group, 16)
    return jnp.concatenate(
        [queries_ref[at, pl.ds(HEAD_SIZE * head, HEAD_SIZE)] for head in range(8)], axis=0
    )


def cached_kernel(lengths_ref, queries_ref, keys_ref, values_ref, sums_ref, stats_ref):
    row = lax.broadcasted_iota(jnp.int32, (128, 128), 0)
    lane = lax.broadcasted_iota(jnp.int32, (128, 128), 1)
    same_row = (row // 4) % 4 == lane // CACHE_SLOTS
    for group in range(16):
        at = pl.ds(128 * group, 128)
        longest = jnp.zeros((128, 128), jnp.int32)
        for k in range(4):
            longest = jnp.where(lane // CACHE_SLOTS == k, lengths_ref[4 * group + k], longest)
        scores = lax.dot_general(
            group_queries(queries_ref, group),
            keys_ref[at, :],
            (((1,), (1,)), ((), ())),
            preferred_element_type=jnp.float32,
        ) * (HEAD_SIZE**-0.5)
        scores = jnp.where(same_row & (lane % CACHE_SLOTS < longest), scores, -jnp.inf)
        top = jnp.max(scores, axis=1, keepdims=True)
        probs = jnp.exp(scores - top)
        total = jnp.sum(probs, axis=1, keepdims=True)
        sums_ref[at, :] = jnp.dot(
            probs.astype(jnp.bfloat16), values_ref[at, :], preferred_element_type=jnp.float32
        )
        stats_ref[:, group : group + 1] = top
        stats_ref[:, 16 + group : 17 + group] = total


def cached_part(lengths, queries, keys, values):
    vmem = pl.BlockSpec(memory_space=pltpu.VMEM)
    return pl.pallas_call(
        cached_kernel,
        in_specs=[pl.BlockSpec(memory_space=pltpu.SMEM), vmem, vmem, vmem],
        out_shape=[
            jax.ShapeDtypeStruct((2048, HEAD_SIZE), jnp.float32),
            jax.ShapeDtypeStruct((128, 128), jnp.float32),
        ],
        compiler_params=pltpu.CompilerParams(vmem_limit_bytes=12 << 20),
        cost_estimate=pl.CostEstimate(flops=150_000_000, bytes_accessed=3 << 20, transcendentals=1 << 18),
        name="cached",
    )(lengths, queries, keys, values)


def finish_kernel(
    parts_ref, cosine_ref, sine_ref, queries_ref, sums_ref, stats_ref, attended_ref, appended_ref
):
    total = jnp.zeros((TOKENS, 256), jnp.float32)
    sums = jnp.zeros((1, TOKENS), jnp.float32)
    for k in range(4):
        total += parts_ref[k, :TOKENS, :].astype(jnp.float32)
        tail = parts_ref[k, TOKENS:, :].astype(jnp.float32)
        sums += tail[0:1] + tail[1:2]
    scale = lax.rsqrt(sums / MODEL_WIDTH + norm_eps)
    scale = jnp.transpose(jnp.broadcast_to(scale, (HEAD_SIZE, TOKENS)))
    keys = total[:, :HEAD_SIZE] * scale
    keys = keys * cosine_ref[...] + pltpu.roll(keys, HEAD_SIZE // 2, 1) * sine_ref[...]
    keys = keys.astype(jnp.bfloat16)
    values = (total[:, HEAD_SIZE:] * scale).astype(jnp.bfloat16)
    appended_ref[:, :, :HEAD_SIZE] = keys.reshape(64, 4, HEAD_SIZE)
    appended_ref[:, :, HEAD_SIZE:] = values.reshape(64, 4, HEAD_SIZE)
    row = lax.broadcasted_iota(jnp.int32, (128, 16), 0)
    lane = lax.broadcasted_iota(jnp.int32, (128, 16), 1)
    seen = ((row // 4) % 4 == lane // 4) & (lane % 4 <= row % 4)
    for group in range(16):
        at = pl.ds(128 * group, 128)
        near = slice(16 * group, 16 * group + 16)
        scores = lax.dot_general(
            group_queries(queries_ref, group),
            keys[near],
            (((1,), (1,)), ((), ())),
            preferred_element_type=jnp.float32,
        ) * (HEAD_SIZE**-0.5)
        scores = jnp.where(seen, scores, -jnp.inf)
        old_top = stats_ref[:, group : group + 1]
        old_total = stats_ref[:, 16 + group : 17 + group]
        top = jnp.maximum(jnp.max(scores, axis=1, keepdims=True), old_top)
        probs = jnp.exp(scores - top)
        factor = jnp.exp(old_top - top)
        denom = jnp.sum(probs, axis=1, keepdims=True) + old_total * factor
        blended = sums_ref[at, :] * factor + jnp.dot(
            probs.astype(jnp.bfloat16), values[near], preferred_element_type=jnp.float32
        )
        blended = (blended / denom).astype(jnp.bfloat16)
        for head in range(8):
            attended_ref[4 * group : 4 * group + 4, :, HEAD_SIZE * head : HEAD_SIZE * (head + 1)] = (
                blended[16 * head : 16 * head + 16].reshape(4, 4, HEAD_SIZE)
            )


def finish(parts, cosine, sine, queries, sums, stats):
    return pl.pallas_call(
        finish_kernel,
        out_shape=[
            jax.ShapeDtypeStruct((TOKENS // 4, 4, SLICE), jnp.bfloat16),
            jax.ShapeDtypeStruct((TOKENS // 4, 4, 256), jnp.bfloat16),
        ],
        compiler_params=pltpu.CompilerParams(vmem_limit_bytes=12 << 20),
        name="finish",
    )(parts, cosine, sine, queries, sums, stats)


def turns(lengths, steps):
    half = HEAD_SIZE // 2
    frequency = rope_base ** (-(jnp.arange(half, dtype=jnp.float32) * 2.0 / HEAD_SIZE))
    positions = (lengths[:, None] + jnp.arange(steps, dtype=jnp.int32)[None, :]).astype(jnp.float32)
    angles = positions.reshape(-1)[:, None] * frequency[None, :]
    cosine, sine = jnp.cos(angles), jnp.sin(angles)
    return jnp.concatenate([cosine, cosine], axis=1), jnp.concatenate([-sine, sine], axis=1)


def along_x(array, shift):
    at = [(x % 2) * 2 + x // 2 for x in range(4)]
    return lax.ppermute(array, ("xl", "xh"), [(at[x], at[(x + shift) % 4]) for x in range(4)])


def along_z(array, shift):
    return lax.ppermute(array, Z, [(z, (z + shift) % 32) for z in range(32)])


def shards(
    tokens,
    norm_gain,
    queries,
    rotated_key_cache,
    head_value_cache,
    lengths,
    master,
    moment_first,
    moment_second,
    gradient,
):
    batch_rows, steps = (tokens.shape[0], tokens.shape[1])
    exchange = [(a * 4 + b, b * 4 + a) for a in range(4) for b in range(4)]
    turned = lax.ppermute(tokens, ("y", "xl", "c"), exchange)
    gain = lax.ppermute(norm_gain.reshape(1, SLICE), ("y", "xl", "c"), exchange)
    turned = prepare(turned.reshape(TOKENS, SLICE), gain)
    average = beta_first * moment_first + (1.0 - beta_first) * gradient
    variance = beta_second * moment_second + (1.0 - beta_second) * gradient * gradient
    update = average / correct_first / (jnp.sqrt(variance / correct_second) + adam_eps)
    renewed = master - learn_rate * (update + decay_rate * master)
    layer_half = renewed.astype(jnp.bfloat16)
    columns = layer_half.shape[1]
    spread = lax.all_to_all(jnp.broadcast_to(layer_half[None], (4, 64, columns)), "far", 0, 0)
    spread = spread.reshape(256, columns)
    ring = []
    for d in (2, 1, 3):
        ring.append(along_x(turned, d))
    own = jnp.stack([turned, ring[1], ring[0], ring[2]])
    other = lax.ppermute(own, "c", [(0, 1), (1, 0)])
    below = along_z(spread, 3)
    above = along_z(spread, 29)
    up, down = joined(spread, below, above)
    from_below = along_z(up, 1)
    from_above = along_z(down, 31)
    queries_flat = queries.reshape(TOKENS, SLICE)
    old_sums, old_stats = cached_part(
        lengths,
        queries_flat,
        rotated_key_cache.reshape(batch_rows * CACHE_SLOTS, HEAD_SIZE),
        head_value_cache.reshape(batch_rows * CACHE_SLOTS, HEAD_SIZE),
    )
    cosine, sine = turns(lengths, steps)
    partial = project(own, other, [up, down, from_below, from_above])
    parts = lax.all_to_all(partial, "y", 0, 0)
    attended, appended = finish(parts, cosine, sine, queries_flat, old_sums, old_stats)
    return (
        attended,
        appended,
        renewed,
        average,
        variance,
    )


def solution(mesh):
    split = Mesh(
        mesh.devices.reshape(4, 4, 8, 2, 2, 2),
        ("y", "far", "near", "xl", "c", "xh"),
    )
    placed = (
        P(GRP, None, COLS),
        P(COLS),
        P(GRP, None, COLS),
        P(GRP, None, COLS),
        P(GRP, None, COLS),
        P(GRP),
        P(GRP, COLS),
        P(GRP, COLS),
        P(GRP, COLS),
        P(GRP, COLS),
    )
    return jax.shard_map(
        shards,
        mesh=split,
        in_specs=placed,
        out_specs=(
            P(GRP, None, COLS),
            P(GRP, None, COLS),
            P(GRP, COLS),
            P(GRP, COLS),
            P(GRP, COLS),
        ),
        check_vma=False,
    )
```
